32 devices in a mesh: dp: 4 (over z), fsdp: 8 (over y, x, core).
Axes of the slice: x: 2, y: 2, z: 4, core: 2. Of those that a mesh axis runs over, the one named last changes fastest.
Arguments:
- hidden: bfloat16 [8192, 4096], P(('dp', 'fsdp')), may hold values from -6 to 6
- queries: bfloat16 [8192, 2048], P(('dp', 'fsdp')), may hold values from -6 to 6
- keys: bfloat16 [8192, 512], P(('dp', 'fsdp')), may hold values from -6 to 6
- target: bfloat16 [8192, 2048], P(('dp', 'fsdp')), may hold values from -6 to 6
- lengths: int32 [32], P(('dp', 'fsdp')), may hold values from 64 to 256
- value_weight_frozen: bfloat16 [4096, 512], P('fsdp'), may hold values from -0.09375 to 0.09375
- adapter_down_map: float32 [4096, 64], P('fsdp'), may hold values from -0.09375 to 0.09375
- adapter_up_map: float32 [64, 512], replicated, may hold values from -0.75 to 0.75
- average_down_map: float32 [4096, 64], P('fsdp'), may hold values from -0.09375 to 0.09375
- average_up_map: float32 [64, 512], replicated, may hold values from -0.75 to 0.75
Outputs:
- down_map_gradient: float32 [4096, 64], P('fsdp')
- up_map_gradient: float32 [64, 512], replicated
- average_down_next: float32 [4096, 64], P('fsdp')
- average_up_next: float32 [64, 512], replicated
- loss: float32 [], replicated
The draws below stay inside these ranges and needn't reach their ends.
Inputs may be any that keep to these rules, and one draw needn't show every extreme that they name: `lengths`: slots at or past a sequence's length are padding.
All inputs are finite; a program needn't handle non-finite values.
Results may differ from the reference program's by a relative error of at most 0.0049.
Values may be sent and summed in bfloat16 or wider, within the bound.
A program may use at most 64 MiB of HBM per device.

```python
import math
import jax
import jax.numpy as jnp
from jax import lax

MODEL_DIM = 4096
HEADS = 16
KEY_VALUE_HEADS = 4
HEAD_DIM = 128
ADAPTER_RANK = 64
TOK_DEV = 256
TOKENS = 8192
DEVICES = 32


def aligned_pair(key):
    base_seed = jax.random.fold_in(key, 7101)
    sign_seed, query_seed, strength_seed, noise_query, noise_keys = jax.random.split(base_seed, 5)
    seq_count = TOKENS // TOK_DEV
    group_size = HEADS // KEY_VALUE_HEADS
    query_field = jnp.clip(jax.random.normal(noise_query, (TOKENS, HEADS * HEAD_DIM), jnp.float32), -6.0, 6.0)
    key_field = jnp.clip(jax.random.normal(noise_keys, (TOKENS, KEY_VALUE_HEADS * HEAD_DIM), jnp.float32), -6.0, 6.0)
    lowest = 4.5
    signs = (2 * jax.random.randint(sign_seed, (seq_count, KEY_VALUE_HEADS, HEAD_DIM), 0, 2) - 1).astype(jnp.float32)
    key_strength = jax.random.uniform(strength_seed, (seq_count, KEY_VALUE_HEADS, 1), jnp.float32, lowest, 6.0)
    query_strength = jax.random.uniform(query_seed, (seq_count, 2, HEADS, 1), jnp.float32, lowest, 6.0)
    score_gap = 1.8 / (5.25 * math.sqrt(HEAD_DIM))
    key_rows = jnp.stack([key_strength * signs, (key_strength - score_gap) * signs], axis=1)
    query_signs = jnp.repeat(signs, group_size, axis=1)
    query_rows = query_strength * query_signs[:, None]
    query_field = query_field.reshape(seq_count, TOK_DEV, HEADS * HEAD_DIM)
    query_field = query_field.at[:, 2:4].set(query_rows.reshape(seq_count, 2, HEADS * HEAD_DIM))
    key_field = key_field.reshape(seq_count, TOK_DEV, KEY_VALUE_HEADS * HEAD_DIM)
    key_field = key_field.at[:, 0:2].set(key_rows.reshape(seq_count, 2, KEY_VALUE_HEADS * HEAD_DIM))
    return (query_field.reshape(TOKENS, HEADS * HEAD_DIM), key_field.reshape(TOKENS, KEY_VALUE_HEADS * HEAD_DIM))


def draw_queries(key, part):
    return aligned_pair(key)[0].astype(jnp.bfloat16)


def draw_keys(key, part):
    return aligned_pair(key)[1].astype(jnp.bfloat16)


def with_ends(array, rng, smallest, high):
    longest = array.shape.index(max(array.shape))
    spots = []
    for shift in (0, 1):
        where = [jax.random.randint(jax.random.fold_in(rng, axis), (), 0, length) for axis, length in enumerate(array.shape)]
        where[longest] = (where[longest] + shift) % array.shape[longest]
        spots.append(tuple(where))
    return array.at[spots[0]].set(smallest).at[spots[1]].set(high)


def block_levels(own_key, shape, cuts, smallest, top_value):
    level = 1.0
    for axis_at, shards_of in cuts:
        draws = jax.random.uniform(jax.random.fold_in(jax.random.fold_in(own_key, 6), axis_at), (shards_of,), jnp.float32, smallest / len(cuts), top_value / len(cuts))
        level = level * jnp.repeat(jnp.exp(draws), shape[axis_at] // shards_of).reshape((-1,) + (1,) * (len(shape) - 1 - axis_at))
    return level


def gaussian(rng, shape, scale, bound, pieces=(), kind=jnp.bfloat16):
    array = scale * jax.random.normal(rng, shape, jnp.float32)
    if pieces:
        array = array * block_levels(rng, shape, pieces, -0.22, 0.18)
    return jnp.clip(array, -bound, bound).astype(kind)


def setup_inputs(seed: int = 0) -> dict:
    streams_of = jax.random.split(jax.random.key(seed), 11)
    return {
        "hidden": gaussian(streams_of[0], (TOKENS, MODEL_DIM), 1.0, 6.0, ((0, 32),)),
        "queries": draw_queries(jax.random.fold_in(streams_of[10], 71), 0),
        "keys": draw_keys(jax.random.fold_in(streams_of[10], 71), 0),
        "target": gaussian(streams_of[3], (TOKENS, HEADS * HEAD_DIM), 1.0, 6.0, ((0, 32),)),
        "lengths": with_ends(jax.random.randint(streams_of[4], (DEVICES,), TOK_DEV // 4, TOK_DEV + 1), jax.random.fold_in(streams_of[4], 1), TOK_DEV // 4, TOK_DEV).astype(jnp.int32),
        "value_weight_frozen": gaussian(streams_of[5], (MODEL_DIM, KEY_VALUE_HEADS * HEAD_DIM), MODEL_DIM ** -0.5, 0.09375, ((0, 8),)),
        "adapter_down_map": gaussian(streams_of[6], (MODEL_DIM, ADAPTER_RANK), MODEL_DIM ** -0.5, 0.09375, ((0, 8),), jnp.float32),
        "adapter_up_map": gaussian(streams_of[7], (ADAPTER_RANK, KEY_VALUE_HEADS * HEAD_DIM), ADAPTER_RANK ** -0.5, 0.75, (), jnp.float32),
        "average_down_map": gaussian(streams_of[8], (MODEL_DIM, ADAPTER_RANK), MODEL_DIM ** -0.5, 0.09375, ((0, 8),), jnp.float32),
        "average_up_map": gaussian(streams_of[9], (ADAPTER_RANK, KEY_VALUE_HEADS * HEAD_DIM), ADAPTER_RANK ** -0.5, 0.75, (), jnp.float32),
    }


adapter_scale = 2.0
average_decay = 0.9
learning_rate = 1.0
masked_score = -1e+30

def per_sequence(items):
    queries, keys, value_outputs, target, seq_length = items
    tok_rows = queries.shape[0]
    group_size = HEADS // KEY_VALUE_HEADS
    position = jnp.arange(tok_rows, dtype=jnp.int32)
    allowed = (position[None, :] <= position[:, None]) & (position[None, :] < seq_length)
    q_heads = queries.reshape(tok_rows, HEADS, HEAD_DIM).astype(jnp.float32)
    k_heads = jnp.repeat(keys.reshape(tok_rows, KEY_VALUE_HEADS, HEAD_DIM), group_size, axis=1).astype(jnp.float32)
    v_heads = jnp.repeat(value_outputs.reshape(tok_rows, KEY_VALUE_HEADS, HEAD_DIM), group_size, axis=1).astype(jnp.float32)
    scores = jnp.einsum('thd,shd->hts', q_heads, k_heads) / math.sqrt(HEAD_DIM)
    scores = jnp.where(allowed[None], scores, masked_score)
    attn_probs = jax.nn.softmax(scores, axis=-1).astype(jnp.bfloat16)
    output = jnp.einsum('hts,shd->thd', attn_probs.astype(jnp.float32), v_heads).reshape(tok_rows, HEADS * HEAD_DIM)
    live_rows = (position < seq_length)[:, None]
    differ = jnp.where(live_rows, output - target.astype(jnp.float32), 0.0)
    loss_part = jnp.sum(differ * differ)
    cotangent = differ.astype(jnp.bfloat16).reshape(tok_rows, HEADS, HEAD_DIM).astype(jnp.float32)
    value_grad = jnp.einsum('hts,thd->shd', attn_probs.astype(jnp.float32), cotangent)
    value_grad = value_grad.reshape(tok_rows, KEY_VALUE_HEADS, group_size, HEAD_DIM).sum(axis=2).reshape(tok_rows, KEY_VALUE_HEADS * HEAD_DIM)
    return (value_grad.astype(jnp.bfloat16), loss_part)

def reference(hidden, queries, keys, target, lengths, value_weight_frozen, adapter_down_map, adapter_up_map, average_down_map, average_up_map):
    down_factor_slice = adapter_down_map.astype(jnp.bfloat16)
    up_factor_slice = adapter_up_map.astype(jnp.bfloat16)
    frozen_value_output = jnp.dot(hidden, value_weight_frozen, preferred_element_type=jnp.float32)
    adapter_hidden = jnp.dot(hidden, down_factor_slice, preferred_element_type=jnp.float32).astype(jnp.bfloat16)
    value_outputs = (frozen_value_output + adapter_scale * jnp.dot(adapter_hidden, up_factor_slice, preferred_element_type=jnp.float32)).astype(jnp.bfloat16)
    token_grand_count = jnp.sum(lengths).astype(jnp.float32)
    value_grad, loss_parts = lax.map(per_sequence, (queries.reshape(DEVICES, TOK_DEV, HEADS * HEAD_DIM), keys.reshape(DEVICES, TOK_DEV, KEY_VALUE_HEADS * HEAD_DIM), value_outputs.reshape(DEVICES, TOK_DEV, KEY_VALUE_HEADS * HEAD_DIM), target.reshape(DEVICES, TOK_DEV, HEADS * HEAD_DIM), lengths))
    value_grad = value_grad.reshape(DEVICES * TOK_DEV, KEY_VALUE_HEADS * HEAD_DIM)
    loss = jnp.sum(loss_parts) / (2.0 * token_grand_count)
    adapter_factor = adapter_scale / token_grand_count
    up_map_gradient = adapter_factor * jnp.dot(adapter_hidden.T, value_grad, preferred_element_type=jnp.float32)
    latent_grad = jnp.dot(value_grad, up_factor_slice.T, preferred_element_type=jnp.float32).astype(jnp.bfloat16)
    down_map_gradient = adapter_factor * jnp.dot(hidden.T, latent_grad, preferred_element_type=jnp.float32)
    average_down_next = average_decay * average_down_map + (1.0 - average_decay) * (adapter_down_map - learning_rate * down_map_gradient)
    average_up_next = average_decay * average_up_map + (1.0 - average_decay) * (adapter_up_map - learning_rate * up_map_gradient)
    return (down_map_gradient, up_map_gradient, average_down_next, average_up_next, loss)
```

```python
import functools
import math

import jax
import jax.numpy as jnp
from jax import lax
from jax.experimental import pallas as pl
from jax.experimental.pallas import tpu as pltpu
from jax.sharding import PartitionSpec as P

HEADS = 16
KEY_VALUE_HEADS = 4
HEAD_DIM = 128
GROUP = HEADS // KEY_VALUE_HEADS

adapter_scale = 2.0
average_decay = 0.9
learning_rate = 1.0
masked_score = -1e30
f32 = jnp.float32
bf16 = jnp.bfloat16


def dot(a, b, dims=((1,), (0,))):
    return lax.dot_general(a, b, (dims, ((), ())), preferred_element_type=f32)


def kernel(
    ndp, nf,
    hid_hbm, q_hbm, k_hbm, tgt_hbm, len_ref, w_hbm, down_ref, up_ref, avd_ref, avu_ref,
    gd_ref, gu_ref, nd_ref, nu_ref, loss_ref,
    hid, qv, kv, tgt, wall, dall, acc, lat, probs, probs_t, cot, vg,
    dpart, dfrom, upart, ufrom, spart, sfrom,
    send2, got2, sc2, send3, got3, sc3, uhalf, uother,
    lsem, g_ss, g_rs, p_ss, p_rs, a_ss, a_rs, b_ss, b_rs, c_ss, c_rs, e_ss, e_rs,
):
    z = lax.axis_index("dp")
    me = lax.axis_index("fsdp")
    chip, core = me // 2, me % 2
    nch = nf // 2
    rows = w_hbm.shape[0]
    rank = up_ref.shape[0]
    width = up_ref.shape[1]
    half = width // 2
    toks = hid.shape[0]
    xor = nch & (nch - 1) == 0

    def toward(d):
        return chip ^ d if xor else lax.rem(chip + d, nch)

    def origin(d):
        return chip ^ d if xor else lax.rem(chip + nch - d, nch)

    def remote(src, dst, ss, rs, fsdp=None, dp=None):
        where = {"fsdp": me if fsdp is None else fsdp, "dp": z if dp is None else dp}
        return pltpu.make_async_remote_copy(
            src_ref=src, dst_ref=dst, send_sem=ss, recv_sem=rs,
            device_id=where, device_id_type=pl.DeviceIdType.MESH,
        )

    partner = 2 * chip + 1 - core

    def rows_of(i):
        return pl.ds(pl.multiple_of(i * rows, rows), rows)

    loads = [
        pltpu.make_async_copy(w_hbm, wall.at[rows_of(me)], lsem.at[0]),
        pltpu.make_async_copy(k_hbm, kv, lsem.at[1]),
        pltpu.make_async_copy(q_hbm, qv, lsem.at[2]),
        pltpu.make_async_copy(hid_hbm, hid, lsem.at[3]),
        pltpu.make_async_copy(tgt_hbm, tgt, lsem.at[4]),
    ]
    for c in loads:
        c.start()

    barrier = pltpu.get_barrier_semaphore()
    pl.semaphore_signal(barrier, inc=1, device_id={"fsdp": partner, "dp": z}, device_id_type=pl.DeviceIdType.MESH)
    for d in range(1, nch):
        pl.semaphore_signal(barrier, inc=1, device_id={"fsdp": 2 * toward(d) + core, "dp": z}, device_id_type=pl.DeviceIdType.MESH)
    for d in range(1, ndp):
        pl.semaphore_signal(barrier, inc=1, device_id={"fsdp": me, "dp": lax.rem(z + d, ndp)}, device_id_type=pl.DeviceIdType.MESH)
    dall[me] = down_ref[...].T.astype(bf16)
    loads[0].wait()
    pl.semaphore_wait(barrier, 1 + (nch - 1) + (ndp - 1))

    sends = []

    def both(i, ss, rs, to):
        out = [
            remote(wall.at[rows_of(i)], wall.at[rows_of(i)], ss.at[0], rs.at[0], fsdp=to),
            remote(dall.at[i], dall.at[i], ss.at[1], rs.at[1], fsdp=to),
        ]
        for c in out:
            c.start()
        sends.extend(out)
        return out

    direct = {d: both(me, g_ss.at[d], g_rs.at[d], 2 * toward(d) + core) for d in range(1, nch)}
    relay = {0: both(me, p_ss.at[0], p_rs.at[0], partner)}

    seq_length = len_ref[0]
    key_at = lax.broadcasted_iota(jnp.int32, (toks, toks), 1)
    query_at = lax.broadcasted_iota(jnp.int32, (toks, toks), 0)
    allowed = (key_at <= query_at) & (key_at < seq_length)
    scale = 1.0 / math.sqrt(HEAD_DIM)
    loads[1].wait()
    loads[2].wait()
    for h in range(HEADS):
        g = h // GROUP
        s = dot(qv[:, h * HEAD_DIM:(h + 1) * HEAD_DIM], kv[:, g * HEAD_DIM:(g + 1) * HEAD_DIM], ((1,), (1,)))
        s = jnp.where(allowed, s, masked_score)
        w = jnp.exp((s - jnp.max(s, axis=1, keepdims=True)) * scale)
        p = (w / jnp.sum(w, axis=1, keepdims=True)).astype(bf16)
        probs[h] = p
        probs_t[h] = p.T
    loads[3].wait()
    loads[4].wait()

    aligned = rows % 128 == 0
    acc[...] = jnp.zeros_like(acc)
    lat[...] = jnp.zeros_like(lat)

    def piece(i, static=False):
        if static:
            x = hid[:, i * rows:(i + 1) * rows]
        else:
            x = hid[:, pl.ds(pl.multiple_of(i * rows, rows), rows)]
        acc[...] += dot(x, wall[rows_of(i), :] if not static else wall[i * rows:(i + 1) * rows, :])
        lat[...] += dot(x, dall[i], ((1,), (1,)))

    if aligned:
        piece(me)
    for d in range(1, nch):
        for c in direct[d]:
            c.wait_recv()
        i = 2 * origin(d) + core
        relay[d] = both(i, p_ss.at[d], p_rs.at[d], partner)
        for c in relay[d - 1]:
            c.wait_recv()
        if aligned:
            piece(i)
            piece(2 * origin(d - 1) + 1 - core)
    for c in relay[nch - 1]:
        c.wait_recv()
    if aligned:
        piece(2 * origin(nch - 1) + 1 - core)
    else:
        for i in range(nf):
            piece(i, True)

    up = up_ref[...].astype(bf16)
    latent = lat[...].astype(bf16)
    values = (acc[...] + adapter_scale * dot(latent, up)).astype(bf16)
    live = lax.broadcasted_iota(jnp.int32, (toks, 1), 0) < seq_length
    total = jnp.zeros((toks, HEAD_DIM), f32)
    for g in range(KEY_VALUE_HEADS):
        v = values[:, g * HEAD_DIM:(g + 1) * HEAD_DIM]
        grad = jnp.zeros((toks, HEAD_DIM), f32)
        for j in range(GROUP):
            h = g * GROUP + j
            differ = dot(probs[h], v) - tgt[:, h * HEAD_DIM:(h + 1) * HEAD_DIM].astype(f32)
            differ = jnp.where(live, differ, 0.0)
            total += differ * differ
            grad += dot(probs_t[h], differ.astype(bf16))
        vg[:, g * HEAD_DIM:(g + 1) * HEAD_DIM] = grad.astype(bf16)
    value_grad = vg[...]
    u = dot(lat[...].T.astype(bf16), value_grad)
    upart[0] = u[:, :half]
    upart[1] = u[:, half:]
    loss_local = jnp.sum(jnp.sum(total, axis=0, keepdims=True), axis=1, keepdims=True)
    count_local = jnp.sum(live.astype(f32), axis=0, keepdims=True)
    row = lax.broadcasted_iota(jnp.int32, spart.shape, 0)
    spart[...] = jnp.where(row == 0, loss_local, count_local)
    lg = dot(up, value_grad, ((1,), (1,))).astype(bf16)
    for i in range(nf):
        dpart[i % 2, i // 2] = dot(lg, hid[:, i * rows:(i + 1) * rows])

    step = [
        remote(dpart.at[1 - core], dfrom, a_ss.at[0], a_rs.at[0], fsdp=partner),
        remote(upart.at[1 - core], ufrom, a_ss.at[1], a_rs.at[1], fsdp=partner),
        remote(spart, sfrom, a_ss.at[2], a_rs.at[2], fsdp=partner),
    ]
    for c in step:
        c.start()
    for c in step:
        c.wait_recv()
    sends.extend(step)
    usum = (upart[core] + ufrom[...]).astype(bf16)
    for q in range(nch):
        send2[q, :, :rows] = (dpart[core, q] + dfrom[q]).astype(bf16)
        send2[q, :, rows:] = usum
    sc2[chip] = spart[...] + sfrom[...]
    got2[chip] = send2[chip]

    step = []
    for d in range(1, nch):
        to = toward(d)
        step.append(remote(send2.at[to], got2.at[chip], b_ss.at[d, 0], b_rs.at[d, 0], fsdp=2 * to + core))
        step.append(remote(sc2.at[chip], sc2.at[chip], b_ss.at[d, 1], b_rs.at[d, 1], fsdp=2 * to + core))
    for c in step:
        c.start()
    for c in step:
        c.wait_recv()
    sends.extend(step)
    t = got2[0].astype(f32)
    s = sc2[0]
    for q in range(1, nch):
        t += got2[q].astype(f32)
        s += sc2[q]
    got3[z] = t.astype(bf16)
    sc3[z] = s

    step = []
    for d in range(1, ndp):
        to = lax.rem(z + d, ndp)
        step.append(remote(got3.at[z], got3.at[z], c_ss.at[d, 0], c_rs.at[d, 0], dp=to))
        step.append(remote(sc3.at[z], sc3.at[z], c_ss.at[d, 1], c_rs.at[d, 1], dp=to))
    for c in step:
        c.start()
    for c in step:
        c.wait_recv()
    sends.extend(step)
    t = got3[0].astype(f32)
    s = sc3[0]
    for q in range(1, ndp):
        t += got3[q].astype(f32)
        s += sc3[q]
    uhalf[...] = t[:, rows:]
    last = remote(uhalf, uother, e_ss, e_rs, fsdp=partner)
    last.start()
    count = s[1:2, 0:1]
    factor = adapter_scale / count
    loss_ref[...] = s[0:1, 0:1] / (2.0 * count)
    gd = (t[:, :rows] * factor).T
    gd_ref[...] = gd
    nd_ref[...] = average_decay * avd_ref[...] + (1.0 - average_decay) * (down_ref[...] - learning_rate * gd)
    last.wait_recv()
    mine, other = uhalf[...], uother[...]
    first = core == 0
    gu = jnp.concatenate([jnp.where(first, mine, other), jnp.where(first, other, mine)], axis=1) * factor
    gu_ref[...] = gu
    nu_ref[...] = average_decay * avu_ref[...] + (1.0 - average_decay) * (up_ref[...] - learning_rate * gu)
    sends.append(last)
    for c in sends:
        c.wait_send()


def per_device(
    ndp, nf,
    hidden, queries, keys, target, lengths,
    value_weight_frozen, adapter_down_map, adapter_up_map, average_down_map, average_up_map,
):
    toks, dim = hidden.shape
    rows, width = value_weight_frozen.shape
    rank = adapter_up_map.shape[0]
    nch = nf // 2
    half = width // 2
    vm = pl.BlockSpec(memory_space=pltpu.VMEM)
    anyspace = pl.BlockSpec(memory_space=pl.ANY)
    shape = jax.ShapeDtypeStruct
    dma = pltpu.SemaphoreType.DMA
    out = pl.pallas_call(
        functools.partial(kernel, ndp, nf),
        out_shape=(
            shape((rows, rank), f32), shape((rank, width), f32),
            shape((rows, rank), f32), shape((rank, width), f32), shape((1, 1), f32),
        ),
        in_specs=[anyspace] * 4 + [pl.BlockSpec(memory_space=pltpu.SMEM), anyspace] + [vm] * 4,
        out_specs=(vm,) * 5,
        scratch_shapes=[
            pltpu.VMEM(hidden.shape, bf16),
            pltpu.VMEM(queries.shape, bf16),
            pltpu.VMEM(keys.shape, bf16),
            pltpu.VMEM(target.shape, bf16),
            pltpu.VMEM((dim, width), bf16),
            pltpu.VMEM((nf, rank, rows), bf16),
            pltpu.VMEM((toks, width), f32),
            pltpu.VMEM((toks, rank), f32),
            pltpu.VMEM((HEADS, toks, toks), bf16),
            pltpu.VMEM((HEADS, toks, toks), bf16),
            pltpu.VMEM((toks, HEAD_DIM), bf16),
            pltpu.VMEM((toks, width), bf16),
            pltpu.VMEM((2, nch, rank, rows), f32),
            pltpu.VMEM((nch, rank, rows), f32),
            pltpu.VMEM((2, rank, half), f32),
            pltpu.VMEM((rank, half), f32),
            pltpu.VMEM((8, 128), f32),
            pltpu.VMEM((8, 128), f32),
            pltpu.VMEM((nch, rank, rows + half), bf16),
            pltpu.VMEM((nch, rank, rows + half), bf16),
            pltpu.VMEM((nch, 8, 128), f32),
            pltpu.VMEM((nch, rank, rows + half), bf16),
            pltpu.VMEM((ndp, rank, rows + half), bf16),
            pltpu.VMEM((ndp, 8, 128), f32),
            pltpu.VMEM((rank, half), f32),
            pltpu.VMEM((rank, half), f32),
            dma((5,)),
            dma((nch, 2)), dma((nch, 2)),
            dma((nch, 2)), dma((nch, 2)),
            dma((3,)), dma((3,)),
            dma((nch, 2)), dma((nch, 2)),
            dma((ndp, 2)), dma((ndp, 2)),
            dma, dma,
        ],
        compiler_params=pltpu.CompilerParams(
            collective_id=0, has_side_effects=True, vmem_limit_bytes=60 * 1024 * 1024
        ),
    )(
        hidden, queries, keys, target, lengths,
        value_weight_frozen, adapter_down_map, adapter_up_map, average_down_map, average_up_map,
    )
    return out[0], out[1], out[2], out[3], out[4].reshape(())


def solution(mesh):
    both = P(("dp", "fsdp"), None)
    placed = (
        both, both, both, both, P(("dp", "fsdp")),
        P("fsdp", None), P("fsdp", None), P(), P("fsdp", None), P(),
    )
    return jax.shard_map(
        functools.partial(per_device, mesh.shape["dp"], mesh.shape["fsdp"]),
        mesh=mesh,
        in_specs=placed,
        out_specs=(P("fsdp", None), P(), P("fsdp", None), P(), P()),
        check_vma=False,
    )
```
